256 devices in a mesh: ent: 128 (over x, y, z_lo, core), grp: 2 (over z_hi).
Axes of the slice: x: 4, y: 4, z: 8 (z_hi: 2, z_lo: 4; z = z_hi * 4 + z_lo), core: 2. Of those that a mesh axis runs over, the one named last changes fastest.
Arguments:
- entity_table: bfloat16 [65536, 1024], P('ent'), may hold values from -2.5 to 2.5
- rel_phases: float32 [822, 512], replicated, may hold values from -3.1416 to 3.1416
- head_ids: int32 [65536], P(('ent', 'grp')), may hold values from 0 to 511
- rel_ids: int32 [65536], P(('ent', 'grp')), may hold values from 0 to 821
- target_pos: int32 [65536], P(('ent', 'grp')), may hold values from 0 to 511
- block_owner: int32 [4], replicated, may hold values from 0 to 127
- block_local: int32 [4], replicated, may hold values from 0 to 3
Outputs:
- losses: float32 [65536], P(('ent', 'grp'))
- head_grad: bfloat16 [65536, 1024], P(('ent', 'grp'))
- table_grad: bfloat16 [65536, 1024], P('ent')
- rel_grad: float32 [822, 512], replicated
The draws below stay inside these ranges and needn't reach their ends.
Inputs may be any that keep to these rules, and one draw needn't show every extreme that they name: query q on device d (ent then grp) has head row (d // 2) * 512 + head_ids[q]. `target_pos`: position among the 512 candidates, block after block. Block b covers table rows from (block_owner[b] * 4 + block_local[b]) * 128 on; blocks may repeat.
All inputs are finite; a program needn't handle non-finite values.
Results may differ from the reference program's by a relative error of at most 0.0057.
Values may be sent and summed in bfloat16 or wider, within the bound.
A program may use at most 64 MiB of HBM per device.

```python
import math
import jax
import jax.numpy as jnp
import numpy as np
from jax import lax

K = 512
R = 822
BLK = 128
NBLK = 4
ENT_DEV = 512
Q_DEV = 256
SHARDS = 128
NENT = 65536
QUERIES = 65536
CAND = 512
N_ENT = 128
N_GRP = 2


def draw_entity_table(key, part):
    key_noise = jax.random.fold_in(key, 2)
    values = jnp.clip(0.25 * jax.random.normal(key_noise, (NENT, 2 * K), jnp.float32), -1.5, 1.5)
    return values.astype(jnp.bfloat16)


def draw_rel_phases(key, part):
    return jax.random.uniform(key, (R, K), jnp.float32, -3.1415, 3.1415)


def plant(values, rng, least, high):
    longest = values.shape.index(max(values.shape))
    spots = []
    for shift in (0, 1):
        where = [jax.random.randint(jax.random.fold_in(rng, axis), (), 0, length) for axis, length in enumerate(values.shape)]
        where[longest] = (where[longest] + shift) % values.shape[longest]
        spots.append(tuple(where))
    return values.at[spots[0]].set(least).at[spots[1]].set(high)


def cumulative_ranks(amount, slope):
    portions = [(1 << 20) // math.isqrt(grade ** slope) + 1 for grade in range(1, amount + 1)]
    width = 1 + sum(portions) // (1 << 30)
    return np.cumsum(np.array([max(1, weight // width) for weight in portions]))


def ranked(key, extent, number_of, lean):
    listing = cumulative_ranks(number_of, lean)
    ticket = jax.random.randint(jax.random.fold_in(key, 1), extent, 0, int(listing[number_of - 1]))
    rank = jnp.searchsorted(jnp.asarray(listing, jnp.int32), ticket, side="right")
    return jax.random.permutation(jax.random.fold_in(key, 2), number_of)[rank].astype(jnp.int32)


def setup_inputs(seed: int = 0) -> dict:
    arg_keys = jax.random.split(jax.random.key(seed), 8)
    return {
        "entity_table": draw_entity_table(jax.random.fold_in(arg_keys[7], 71), 0),
        "rel_phases": draw_rel_phases(jax.random.fold_in(arg_keys[7], 71), 0),
        "head_ids": plant(jax.random.randint(arg_keys[2], (QUERIES,), 0, ENT_DEV), jax.random.fold_in(arg_keys[2], 1), 0, ENT_DEV - 1).astype(jnp.int32),
        "rel_ids": plant(ranked(arg_keys[3], (QUERIES,), R, 2), jax.random.fold_in(arg_keys[3], 3), 0, R - 1).astype(jnp.int32),
        "target_pos": plant(jax.random.randint(arg_keys[4], (QUERIES,), 0, CAND), jax.random.fold_in(arg_keys[4], 1), 0, CAND - 1).astype(jnp.int32),
        "block_owner": plant(jax.random.randint(arg_keys[5], (NBLK,), 0, SHARDS), jax.random.fold_in(arg_keys[5], 1), 0, SHARDS - 1).astype(jnp.int32),
        "block_local": plant(jax.random.randint(arg_keys[6], (NBLK,), 0, ENT_DEV // BLK), jax.random.fold_in(arg_keys[6], 1), 0, (ENT_DEV // BLK) - 1).astype(jnp.int32),
    }


SOFTMAX_TEMPER = 2.0


def device_terms(heads, angles, targets, candidate_block, candidate_norm):
    half_dim = angles.shape[1]
    real_head = heads[:, :half_dim]
    imag_head = heads[:, half_dim:]
    cosine = jnp.cos(angles)
    sine = jnp.sin(angles)
    real_query = real_head * cosine - imag_head * sine
    imag_query = real_head * sine + imag_head * cosine
    query_reduced_precision = jnp.concatenate([real_query, imag_query], axis=1).astype(jnp.bfloat16)
    query_reduced_precision = lax.optimization_barrier(query_reduced_precision).astype(jnp.float32)
    logit_scores = (2.0 * jnp.dot(query_reduced_precision, candidate_block.T, precision=lax.Precision.HIGHEST) - candidate_norm[None, :]) / SOFTMAX_TEMPER
    top = jnp.max(logit_scores, axis=1, keepdims=True)
    log_total = top[:, 0] + jnp.log(jnp.sum(jnp.exp(logit_scores - top), axis=1))
    picked = jnp.take_along_axis(logit_scores, targets[:, None], axis=1)[:, 0]
    losses = log_total - picked
    columns = jnp.arange(logit_scores.shape[1], dtype=jnp.int32)
    onehot = (columns[None, :] == targets[:, None]).astype(jnp.float32)
    softmax_weights = jnp.exp(logit_scores - log_total[:, None]) - onehot
    weights_reduced_precision = lax.optimization_barrier(softmax_weights.astype(jnp.bfloat16)).astype(jnp.float32)
    query_gradient = (2.0 / SOFTMAX_TEMPER) * jnp.dot(weights_reduced_precision, candidate_block, precision=lax.Precision.HIGHEST)
    candidate_gradient = (2.0 / SOFTMAX_TEMPER) * (jnp.dot(weights_reduced_precision.T, query_reduced_precision, precision=lax.Precision.HIGHEST) - jnp.sum(softmax_weights, axis=0)[:, None] * candidate_block)
    real_grad = query_gradient[:, :half_dim]
    imag_grad = query_gradient[:, half_dim:]
    head_grad = jnp.concatenate([real_grad * cosine + imag_grad * sine, imag_grad * cosine - real_grad * sine], axis=1).astype(jnp.bfloat16)
    angle_grad = imag_grad * real_query - real_grad * imag_query
    return losses, head_grad, angle_grad, candidate_gradient


def reference(entity_table, rel_phases, head_ids, rel_ids, target_pos, block_owner, block_local):
    half_dim = rel_phases.shape[1]
    rel_count = rel_phases.shape[0]
    devices = N_ENT * N_GRP
    starts = (block_owner * (ENT_DEV // BLK) + block_local) * BLK
    rows = (starts[:, None] + jnp.arange(BLK, dtype=jnp.int32)[None, :]).reshape(-1).astype(jnp.int32)
    candidate_block = entity_table[rows].astype(jnp.float32)
    candidate_norm = jnp.sum(candidate_block * candidate_block, axis=1)

    def step(carry, inputs):
        cand_total, rel_total = carry
        head_local, rel_local, target_local, device = inputs
        head_rows = ((device // N_GRP) * ENT_DEV + head_local).astype(jnp.int32)
        heads = entity_table[head_rows].astype(jnp.float32)
        angles = rel_phases[rel_local]
        losses, head_grad, angle_grad, candidate_gradient = device_terms(heads, angles, target_local, candidate_block, candidate_norm)
        rel_part = jax.ops.segment_sum(angle_grad, rel_local, num_segments=rel_count)
        return (cand_total + candidate_gradient, rel_total + rel_part), (losses, head_grad)

    start_carry = (jnp.zeros((NBLK * BLK, 2 * half_dim), jnp.float32), jnp.zeros((rel_count, half_dim), jnp.float32))
    inputs = (head_ids.reshape(devices, Q_DEV), rel_ids.reshape(devices, Q_DEV), target_pos.reshape(devices, Q_DEV), jnp.arange(devices, dtype=jnp.int32))
    (cand_total, rel_grad), (losses, head_grad) = lax.scan(step, start_carry, inputs)
    table_grad = jax.ops.segment_sum(cand_total, rows, num_segments=NENT).astype(jnp.bfloat16)
    return losses.reshape(-1), head_grad.reshape(-1, 2 * half_dim), table_grad, rel_grad
```

```python
import jax
import jax.numpy as jnp
from jax import lax
from jax.experimental import pallas as pl
from jax.experimental.pallas import tpu as pltpu
from jax.sharding import Mesh
from jax.sharding import PartitionSpec as P

BLK = 128
ENT = ("x", "y", "zl", "c")
ENT_GRP = ("x", "y", "zl", "c", "zh")
MESH = pl.DeviceIdType.MESH
BF = jnp.bfloat16
F32 = jnp.float32
SOFTMAX_TEMPER = 2.0
RELP = 832
RY = 208


class Spot:
    def __init__(self):
        self.x = lax.axis_index("x")
        self.y = lax.axis_index("y")
        self.c = lax.axis_index("c")
        self.zl = lax.axis_index("zl")
        self.zh = lax.axis_index("zh")
        self.z = self.zh * 4 + self.zl

    def xs(self, k):
        t = lax.rem(self.x + k, 4)
        return t, {"x": t}

    def ys(self, k):
        t = lax.rem(self.y + k, 4)
        return t, {"y": t}

    def zs(self, k):
        t = lax.rem(self.z + k, 8)
        return t, {"zh": lax.div(t, 4), "zl": lax.rem(t, 4)}

    def partner(self):
        return {"c": 1 - self.c}

    def greet(self):
        barrier = pltpu.get_barrier_semaphore()
        peers = [self.partner()]
        peers += [self.xs(k)[1] for k in range(1, 4)]
        peers += [self.ys(k)[1] for k in range(1, 4)]
        peers += [self.zs(k)[1] for k in range(1, 8)]
        for peer in peers:
            pl.semaphore_signal(barrier, inc=1, device_id=peer, device_id_type=MESH)
        pl.semaphore_wait(barrier, len(peers))


class Links:
    def __init__(self, send, recv):
        self.send, self.recv, self.used, self.sent = send, recv, 0, []

    def go(self, src, dst, device):
        n = self.used
        self.used += 1
        copy = pltpu.make_async_remote_copy(
            src_ref=src, dst_ref=dst, send_sem=self.send.at[n], recv_sem=self.recv.at[n],
            device_id=device, device_id_type=MESH,
        )
        copy.start()
        self.sent.append(copy)
        return copy

    def drain(self):
        for copy in self.sent:
            copy.wait_send()


def tile(start, size, unit):
    return pl.ds(pl.multiple_of(start, unit), size)


N_BCAST = 64


def bcast_kernel(owner_s, local_s, table_hbm, cand_hbm, table_v, stage, pbuf, sel, r0, r1, t0, t1,
                 q0, q1, zb, cand, send, recv, sem):
    me = Spot()
    x, y, z, c = me.x, me.y, me.z, me.c
    fetch = pltpu.make_async_copy(table_hbm, table_v, sem.at[0])
    fetch.start()
    me.greet()
    fetch.wait()
    links = Links(send, recv)
    entity = ((x * 4 + y) * 4 + me.zl) * 2 + c
    for j in range(2):
        b = me.zh * 2 + j
        held = (owner_s[b] == entity).astype(jnp.int32)
        masks = [
            (held * (local_s[b] == n).astype(jnp.int32)).astype(F32).astype(BF) for n in range(4)
        ]
        for r in range(0, BLK, 16):
            total = table_v[pl.ds(r, 16), :] * masks[0]
            for n in range(1, 4):
                total = total + table_v[pl.ds(n * BLK + r, 16), :] * masks[n]
            stage[j, pl.ds(r, 16), :] = total
    swaps = [
        links.go(stage.at[j, tile((1 - c) * 64, 64, 64), :], pbuf.at[j], me.partner())
        for j in range(2)
    ]
    for j in range(2):
        swaps[j].wait_recv()
        sel[j] = stage[j, tile(c * 64, 64, 64), :] + pbuf[j]
    first = [[], []]
    for k in range(1, 4):
        to, dev = me.xs(k)
        first[0].append(links.go(sel.at[0, :, tile(to * 256, 256, 256)], r0.at[k], dev))
        to, dev = me.ys(k)
        first[1].append(links.go(sel.at[1, tile(to * 16, 16, 16), :], r1.at[k], dev))
    r0[0] = sel[0, :, tile(x * 256, 256, 256)]
    r1[0] = sel[1, tile(y * 16, 16, 16), :]
    for copy in first[0]:
        copy.wait_recv()
    t0[...] = (r0[0] + r0[1]) + (r0[2] + r0[3])
    second = [[], []]
    for k in range(1, 4):
        to, dev = me.ys(k)
        second[0].append(links.go(t0.at[tile(to * 16, 16, 16), :], q0.at[k], dev))
    q0[0] = t0[tile(y * 16, 16, 16), :]
    for copy in first[1]:
        copy.wait_recv()
    t1[...] = (r1[0] + r1[1]) + (r1[2] + r1[3])
    for k in range(1, 4):
        to, dev = me.xs(k)
        second[1].append(links.go(t1.at[:, tile(to * 256, 256, 256)], q1.at[k], dev))
    q1[0] = t1[:, tile(x * 256, 256, 256)]
    for copy in second[0]:
        copy.wait_recv()
    zb[0, 0] = (q0[0] + q0[1]) + (q0[2] + q0[3])
    for copy in second[1]:
        copy.wait_recv()
    zb[0, 1] = (q1[0] + q1[1]) + (q1[2] + q1[3])
    third = []
    for k in range(1, 8):
        to, dev = me.zs(k)
        third.append(links.go(zb.at[0], zb.at[k], dev))
    for copy in third:
        copy.wait_recv()
    here = (tile(c * 64 + y * 16, 16, 16), tile(x * 256, 256, 256))
    zeros = jnp.zeros((16, 256), BF)
    for j in range(2):
        half = [zeros, zeros]
        for k in range(8):
            isl = (lax.rem(z - k + 8, 8) < 4).astype(jnp.int32)
            low = isl.astype(F32).astype(BF)
            high = (1 - isl).astype(F32).astype(BF)
            piece = zb[k, j]
            half[0] = half[0] + piece * low
            half[1] = half[1] + piece * high
        for h in range(2):
            cand[h, j, here[0], here[1]] = half[h]
    fourth = [[], []]
    for k in range(1, 4):
        spot = cand.at[:, 0, here[0], here[1]]
        fourth[0].append(links.go(spot, spot, me.ys(k)[1]))
        spot = cand.at[:, 1, here[0], here[1]]
        fourth[1].append(links.go(spot, spot, me.xs(k)[1]))
    fifth = [[], []]
    forward = [[], []]

    def slab0(xx):
        return cand.at[:, 0, tile(c * 64, 64, 64), tile(xx * 256, 256, 256)]

    def slab1(yy):
        return cand.at[:, 1, tile(c * 64 + yy * 16, 16, 16), :]

    for copy in fourth[0]:
        copy.wait_recv()
    for k in range(1, 4):
        fifth[0].append(links.go(slab0(x), slab0(x), me.xs(k)[1]))
    for copy in fourth[1]:
        copy.wait_recv()
    for k in range(1, 4):
        fifth[1].append(links.go(slab1(y), slab1(y), me.ys(k)[1]))
    forward[0].append(links.go(slab0(x), slab0(x), me.partner()))
    forward[1].append(links.go(slab1(y), slab1(y), me.partner()))
    for k in (1, 3, 2):
        fifth[0][k - 1].wait_recv()
        xx = lax.rem(x - k + 4, 4)
        forward[0].append(links.go(slab0(xx), slab0(xx), me.partner()))
        fifth[1][k - 1].wait_recv()
        yy = lax.rem(y - k + 4, 4)
        forward[1].append(links.go(slab1(yy), slab1(yy), me.partner()))
    for j in range(2):
        for copy in forward[j]:
            copy.wait_recv()
    out = pltpu.make_async_copy(cand, cand_hbm, sem.at[1])
    out.start()
    links.drain()
    out.wait()


def broadcast(owner, local, table):
    smem = pl.BlockSpec(memory_space=pltpu.SMEM)
    anyw = pl.BlockSpec(memory_space=pl.ANY)
    return pl.pallas_call(
        bcast_kernel,
        out_shape=jax.ShapeDtypeStruct((2, 2, 128, 1024), BF),
        in_specs=[smem, smem, anyw],
        out_specs=anyw,
        scratch_shapes=[
            pltpu.VMEM((512, 1024), BF),
            pltpu.VMEM((2, 128, 1024), BF),
            pltpu.VMEM((2, 64, 1024), BF),
            pltpu.VMEM((2, 64, 1024), BF),
            pltpu.VMEM((4, 64, 256), BF),
            pltpu.VMEM((4, 16, 1024), BF),
            pltpu.VMEM((64, 256), BF),
            pltpu.VMEM((16, 1024), BF),
            pltpu.VMEM((4, 16, 256), BF),
            pltpu.VMEM((4, 16, 256), BF),
            pltpu.VMEM((8, 2, 16, 256), BF),
            pltpu.VMEM((2, 2, 128, 1024), BF),
            pltpu.SemaphoreType.DMA((N_BCAST,)),
            pltpu.SemaphoreType.DMA((N_BCAST,)),
            pltpu.SemaphoreType.DMA((2,)),
        ],
        compiler_params=pltpu.CompilerParams(collective_id=0, has_side_effects=True),
    )(owner, local, table)


N_RED = 72


def reduce_kernel(a_ref, b_ref, ga_hbm, gb_hbm, pa, pb, a1, b1, ra, rb, a2, b2, ra2, rb2, a3, b3,
                  raz, rbz, ga, gb, send, recv, sem):
    me = Spot()
    x, y, z, c = me.x, me.y, me.z, me.c
    me.greet()
    links = Links(send, recv)
    swap_a = links.go(a_ref.at[tile((1 - c) * 256, 256, 256), :], pa, me.partner())
    swap_b = links.go(b_ref.at[:, tile((1 - c) * 256, 256, 256)], pb, me.partner())
    swap_a.wait_recv()
    a1[...] = (a_ref[tile(c * 256, 256, 256), :].astype(F32) + pa[...].astype(F32)).astype(BF)
    one_a, one_b = [], []
    for k in (2, 1, 3):
        to, dev = me.xs(k)
        one_a.append(links.go(a1.at[:, tile(to * 256, 256, 256)], ra.at[k - 1], dev))
    swap_b.wait_recv()
    b1[...] = (b_ref[:, tile(c * 256, 256, 256)].astype(F32) + pb[...].astype(F32)).astype(BF)
    for k in (2, 1, 3):
        to, dev = me.ys(k)
        one_b.append(links.go(b1.at[tile(to * RY, RY, 16), :], rb.at[k - 1], dev))
    for copy in one_a:
        copy.wait_recv()
    total = a1[:, tile(x * 256, 256, 256)].astype(F32)
    for k in range(3):
        total = total + ra[k].astype(F32)
    a2[...] = total.astype(BF)
    two_a, two_b = [], []
    for k in (2, 1, 3):
        to, dev = me.ys(k)
        two_a.append(links.go(a2.at[tile(to * 64, 64, 64), :], ra2.at[k - 1], dev))
    for copy in one_b:
        copy.wait_recv()
    total = b1[tile(y * RY, RY, 16), :].astype(F32)
    for k in range(3):
        total = total + rb[k].astype(F32)
    b2[pl.ds(0, RY), :] = total.astype(BF)
    b2[pl.ds(RY, 256 - RY), :] = jnp.zeros((256 - RY, 256), BF)
    for k in (2, 1, 3):
        to, dev = me.xs(k)
        two_b.append(links.go(b2.at[tile(to * 64, 64, 64), :], rb2.at[k - 1], dev))

    def zcell(t):
        return tile(lax.div(t, 2) * 16, 16, 16), tile(lax.rem(t, 2) * 128, 128, 128)

    three_a, three_b = [], []
    for copy in two_a:
        copy.wait_recv()
    total = a2[tile(y * 64, 64, 64), :].astype(F32)
    for k in range(3):
        total = total + ra2[k].astype(F32)
    a3[...] = total.astype(BF)
    for k in (4, 3, 5, 2, 6, 1, 7):
        to, dev = me.zs(k)
        three_a.append(links.go(a3.at[zcell(to)], raz.at[k - 1], dev))
    for copy in two_b:
        copy.wait_recv()
    total = b2[tile(x * 64, 64, 64), :].astype(F32)
    for k in range(3):
        total = total + rb2[k].astype(F32)
    b3[...] = total.astype(BF)
    for k in (4, 3, 5, 2, 6, 1, 7):
        to, dev = me.zs(k)
        three_b.append(links.go(b3.at[zcell(to)], rbz.at[k - 1], dev))

    zr, zc = lax.div(z, 2) * 16, lax.rem(z, 2) * 128

    def a_cell():
        return ga.at[tile(c * 256 + y * 64 + zr, 16, 16), tile(x * 256 + zc, 128, 128)]

    def b_cell():
        return gb.at[y, tile(x * 64 + zr, 16, 16), tile(c * 256 + zc, 128, 128)]

    four_a, four_b = [], []
    for copy in three_a:
        copy.wait_recv()
    total = a3[zcell(z)].astype(F32)
    for k in range(7):
        total = total + raz[k].astype(F32)
    a_cell()[...] = total.astype(BF)
    for k in (4, 3, 5, 2, 6, 1, 7):
        four_a.append(links.go(a_cell(), a_cell(), me.zs(k)[1]))
    for copy in three_b:
        copy.wait_recv()
    total = b3[zcell(z)].astype(F32)
    for k in range(7):
        total = total + rbz[k].astype(F32)
    b_cell()[...] = total.astype(BF)
    for k in (4, 3, 5, 2, 6, 1, 7):
        four_b.append(links.go(b_cell(), b_cell(), me.zs(k)[1]))

    five_a, five_b = [], []
    for copy in four_a:
        copy.wait_recv()
    spot = ga.at[tile(c * 256 + y * 64, 64, 64), tile(x * 256, 256, 256)]
    for k in (2, 1, 3):
        five_a.append(links.go(spot, spot, me.ys(k)[1]))
    for copy in four_b:
        copy.wait_recv()
    spot = gb.at[y, tile(x * 64, 64, 64), tile(c * 256, 256, 256)]
    for k in (2, 1, 3):
        five_b.append(links.go(spot, spot, me.xs(k)[1]))

    def slab_a(xx):
        return ga.at[tile(c * 256, 256, 256), tile(xx * 256, 256, 256)]

    def slab_b(yy):
        return gb.at[yy, pl.ds(0, RY), tile(c * 256, 256, 256)]

    six_a, six_b, last = {}, {}, []
    for copy in five_a:
        copy.wait_recv()
    for k in (2, 1, 3):
        six_a[k] = links.go(slab_a(x), slab_a(x), me.xs(k)[1])
    last.append(links.go(slab_a(x), slab_a(x), me.partner()))
    for copy in five_b:
        copy.wait_recv()
    for k in (2, 1, 3):
        six_b[k] = links.go(slab_b(y), slab_b(y), me.ys(k)[1])
    last.append(links.go(slab_b(y), slab_b(y), me.partner()))
    for k in (1, 3, 2):
        six_a[k].wait_recv()
        xx = lax.rem(x - k + 4, 4)
        last.append(links.go(slab_a(xx), slab_a(xx), me.partner()))
        six_b[k].wait_recv()
        yy = lax.rem(y - k + 4, 4)
        last.append(links.go(slab_b(yy), slab_b(yy), me.partner()))
    for copy in last:
        copy.wait_recv()
    outs = [
        pltpu.make_async_copy(ga, ga_hbm, sem.at[0]),
        pltpu.make_async_copy(gb.at[:, pl.ds(0, RY), :], gb_hbm, sem.at[1]),
    ]
    for copy in outs:
        copy.start()
    links.drain()
    for copy in outs:
        copy.wait()


def all_reduce(a, b):
    anyw = pl.BlockSpec(memory_space=pl.ANY)
    vmem = pl.BlockSpec(memory_space=pltpu.VMEM)
    return pl.pallas_call(
        reduce_kernel,
        out_shape=(
            jax.ShapeDtypeStruct((512, 1024), BF),
            jax.ShapeDtypeStruct((4, RY, 512), BF),
        ),
        in_specs=[vmem, vmem],
        out_specs=(anyw, anyw),
        scratch_shapes=[
            pltpu.VMEM((256, 1024), BF),
            pltpu.VMEM((RELP, 256), BF),
            pltpu.VMEM((256, 1024), BF),
            pltpu.VMEM((RELP, 256), BF),
            pltpu.VMEM((3, 256, 256), BF),
            pltpu.VMEM((3, RY, 256), BF),
            pltpu.VMEM((256, 256), BF),
            pltpu.VMEM((256, 256), BF),
            pltpu.VMEM((3, 64, 256), BF),
            pltpu.VMEM((3, 64, 256), BF),
            pltpu.VMEM((64, 256), BF),
            pltpu.VMEM((64, 256), BF),
            pltpu.VMEM((7, 16, 128), BF),
            pltpu.VMEM((7, 16, 128), BF),
            pltpu.VMEM((512, 1024), BF),
            pltpu.VMEM((4, 256, 512), BF),
            pltpu.SemaphoreType.DMA((N_RED,)),
            pltpu.SemaphoreType.DMA((N_RED,)),
            pltpu.SemaphoreType.DMA((2,)),
        ],
        compiler_params=pltpu.CompilerParams(collective_id=1, has_side_effects=True),
    )(a, b)


def body(entity_table, rel_phases, head_ids, rel_ids, target_pos, block_owner, block_local):
    half_dim = rel_phases.shape[1]
    rel_count = rel_phases.shape[0]
    shard_rows = entity_table.shape[0]
    blocks_total = block_owner.shape[0]
    fetched = broadcast(block_owner, block_local, entity_table)
    candidate_block = fetched.reshape(blocks_total * BLK, 2 * half_dim)
    heads = jnp.take(entity_table, head_ids, axis=0).astype(jnp.float32)
    angles = jnp.take(rel_phases, rel_ids, axis=0)
    cosine = jnp.cos(angles)
    sine = jnp.sin(angles)
    real_head = heads[:, :half_dim]
    imag_head = heads[:, half_dim:]
    real_query = real_head * cosine - imag_head * sine
    imag_query = real_head * sine + imag_head * cosine
    query_reduced_precision = jnp.concatenate([real_query, imag_query], axis=1).astype(jnp.bfloat16)
    candidate_norm = jnp.sum(jnp.square(candidate_block.astype(jnp.float32)), axis=1)
    inner_products = lax.dot_general(
        query_reduced_precision,
        candidate_block,
        (((1,), (1,)), ((), ())),
        preferred_element_type=jnp.float32,
    )
    logit_scores = (2.0 * inner_products - candidate_norm[None, :]) / SOFTMAX_TEMPER
    top = jnp.max(logit_scores, axis=1, keepdims=True)
    log_total = top[:, 0] + jnp.log(jnp.sum(jnp.exp(logit_scores - top), axis=1))
    picked = jnp.take_along_axis(logit_scores, target_pos[:, None], axis=1)[:, 0]
    losses = log_total - picked
    columns = jnp.arange(logit_scores.shape[1], dtype=jnp.int32)
    onehot = (columns[None, :] == target_pos[:, None]).astype(jnp.float32)
    softmax_weights = jnp.exp(logit_scores - log_total[:, None]) - onehot
    weights_reduced_precision = softmax_weights.astype(jnp.bfloat16)
    query_gradient = (
        2.0
        / SOFTMAX_TEMPER
        * jnp.dot(weights_reduced_precision, candidate_block, preferred_element_type=jnp.float32)
    )
    back_products = lax.dot_general(
        weights_reduced_precision,
        query_reduced_precision,
        (((0,), (0,)), ((), ())),
        preferred_element_type=jnp.float32,
    )
    candidate_gradient = (
        2.0
        / SOFTMAX_TEMPER
        * (
            back_products
            - jnp.sum(softmax_weights, axis=0)[:, None] * candidate_block.astype(jnp.float32)
        )
    )
    real_grad = query_gradient[:, :half_dim]
    imag_grad = query_gradient[:, half_dim:]
    head_grad = jnp.concatenate(
        [real_grad * cosine + imag_grad * sine, imag_grad * cosine - real_grad * sine], axis=1
    ).astype(jnp.bfloat16)
    angle_grad = imag_grad * real_query - real_grad * imag_query
    rel_part = jax.ops.segment_sum(angle_grad, rel_ids, num_segments=RELP)
    summed, rel_sum = all_reduce(candidate_gradient.astype(BF), rel_part.astype(BF))
    rel_grad = rel_sum.reshape(RELP, half_dim)[:rel_count].astype(F32)
    block_numbers = jnp.arange(shard_rows // BLK, dtype=jnp.int32)
    selector = (
        (block_owner == lax.axis_index(ENT))[:, None]
        & (block_local[:, None] == block_numbers[None, :])
    )
    blocks = summed.reshape(blocks_total, 1, BLK, 2 * half_dim).astype(F32)
    placed = jnp.sum(jnp.where(selector[:, :, None, None], blocks, 0.0), axis=0)
    table_grad = placed.reshape(shard_rows, 2 * half_dim).astype(jnp.bfloat16)
    return (losses, head_grad, table_grad, rel_grad)


def solution(mesh):
    finer = Mesh(mesh.devices.reshape(4, 4, 4, 2, mesh.shape["grp"]), ENT_GRP)
    placed = (P(ENT, None), P(), P(ENT_GRP), P(ENT_GRP), P(ENT_GRP), P(), P())
    return jax.shard_map(
        body,
        mesh=finer,
        in_specs=placed,
        out_specs=(P(ENT_GRP), P(ENT_GRP, None), P(ENT, None), P()),
        check_vma=False,
    )
```

```python
import jax
import jax.numpy as jnp
from jax import lax
from jax.experimental import pallas as pl
from jax.experimental.pallas import tpu as pltpu
from jax.sharding import Mesh
from jax.sharding import PartitionSpec as P

BLK = 128
ENT = ("x", "y", "zl", "c")
ENT_GRP = ("x", "y", "zl", "c", "zh")
MESH = pl.DeviceIdType.MESH
BF = jnp.bfloat16
F32 = jnp.float32
SOFTMAX_TEMPER = 2.0
RELP = 832
RY = 208


class Spot:
    def __init__(self):
        self.x = lax.axis_index("x")
        self.y = lax.axis_index("y")
        self.c = lax.axis_index("c")
        self.zl = lax.axis_index("zl")
        self.zh = lax.axis_index("zh")
        self.z = self.zh * 4 + self.zl

    def xs(self, k):
        t = lax.rem(self.x + k, 4)
        return t, {"x": t}

    def ys(self, k):
        t = lax.rem(self.y + k, 4)
        return t, {"y": t}

    def zs(self, k):
        t = lax.rem(self.z + k, 8)
        return t, {"zh": lax.div(t, 4), "zl": lax.rem(t, 4)}

    def partner(self):
        return {"c": 1 - self.c}

    def hello(self):
        barrier = pltpu.get_barrier_semaphore()
        peers = [self.partner()]
        peers += [self.xs(k)[1] for k in range(1, 4)]
        peers += [self.ys(k)[1] for k in range(1, 4)]
        peers += [self.zs(k)[1] for k in range(1, 8)]
        for peer in peers:
            pl.semaphore_signal(barrier, inc=1, device_id=peer, device_id_type=MESH)

    def everyone(self):
        pl.semaphore_wait(pltpu.get_barrier_semaphore(), 14)


class Links:
    def __init__(self, send, recv):
        self.send, self.recv, self.used, self.sent = send, recv, 0, []

    def go(self, src, dst, device):
        n = self.used
        self.used += 1
        copy = pltpu.make_async_remote_copy(
            src_ref=src, dst_ref=dst, send_sem=self.send.at[n], recv_sem=self.recv.at[n],
            device_id=device, device_id_type=MESH,
        )
        copy.start()
        self.sent.append(copy)
        return copy

    def drain(self):
        for copy in self.sent:
            copy.wait_send()


def tile(start, size, unit):
    return pl.ds(pl.multiple_of(start, unit), size)


RELK = 896
N_COPY = 112


def lanes_of(row):
    return jnp.transpose(jnp.broadcast_to(row.astype(F32), (128, 256)))


def dot(a, b):
    return jnp.dot(a, b, preferred_element_type=F32)


def step_kernel(owner_s, local_s, head_r, rel_r, target_r, table_hbm, phase_hbm,
                loss_o, head_o, ga, gb,
                table_v, phase_v, tail_v, ph0, ph1, ph2, ohh, ohr, q_v, qr_v, qi_v, cos_v, sin_v,
                stage, pbuf, sel, r0, r1, t0, t1, q0, q1, zb, cand,
                s_v, w_v, wt_v, sum_v, ang0, ang1, oht,
                asend, afull, pa, bsend, bfull, pb, a1, b1, ra, rb, a2f, b2f, a2, b2, ra2, rb2,
                a3f, b3f, a3, b3, raz, rbz, send, recv, sem):
    me = Spot()
    x, y, z, c = me.x, me.y, me.z, me.c
    fetch = pltpu.make_async_copy(table_hbm, table_v, sem.at[0])
    fetch.start()
    fetch_phase = pltpu.make_async_copy(phase_hbm, phase_v, sem.at[1])
    fetch_phase.start()
    me.hello()
    fetch.wait()
    links = Links(send, recv)
    entity = ((x * 4 + y) * 4 + me.zl) * 2 + c
    for j in range(2):
        b = me.zh * 2 + j
        held = (owner_s[b] == entity).astype(jnp.int32)
        masks = [
            (held * (local_s[b] == n).astype(jnp.int32)).astype(F32).astype(BF) for n in range(4)
        ]
        for r in range(0, BLK, 16):
            total = table_v[pl.ds(r, 16), :] * masks[0]
            for n in range(1, 4):
                total = total + table_v[pl.ds(n * BLK + r, 16), :] * masks[n]
            stage[j, pl.ds(r, 16), :] = total
    me.everyone()
    swaps = [
        links.go(stage.at[j, tile((1 - c) * 64, 64, 64), :], pbuf.at[j], me.partner())
        for j in range(2)
    ]

    def prepare():
        lane = lax.broadcasted_iota(jnp.int32, (256, 128), 1).astype(F32)
        ids = lanes_of(head_r[...])
        for g in range(4):
            ohh[:, pl.ds(g * 128, 128)] = (ids == lane + float(g * 128)).astype(F32).astype(BF)
        ids = lanes_of(rel_r[...])
        for g in range(7):
            ohr[:, pl.ds(g * 128, 128)] = (ids == lane + float(g * 128)).astype(F32).astype(BF)

    def split_phases():
        fetch_phase.wait()
        tail_v[...] = jnp.zeros((128, 512), F32)
        tail_v[pl.ds(0, 822 - 768), :] = phase_v[pl.ds(768, 822 - 768), :]
        for r in range(0, RELK, 128):
            rows = pl.ds(r, 128)
            value = phase_v[rows, :] if r < 768 else tail_v[...]
            top = value.astype(BF)
            value = value - top.astype(F32)
            ph0[rows, :] = top
            top = value.astype(BF)
            ph1[rows, :] = top
            ph2[rows, :] = (value - top.astype(F32)).astype(BF)

    def rotate(j):
        cols, more = pl.ds(j * 128, 128), pl.ds(512 + j * 128, 128)
        which = ohr[...]
        theta = dot(which, ph0[:, cols]) + (dot(which, ph1[:, cols]) + dot(which, ph2[:, cols]))
        cosine, sine = jnp.cos(theta), jnp.sin(theta)
        hr = dot(ohh[...], table_v[:, cols])
        hi = dot(ohh[...], table_v[:, more])
        qr = hr * cosine - hi * sine
        qi = hr * sine + hi * cosine
        cos_v[:, cols] = cosine
        sin_v[:, cols] = sine
        qr_v[:, cols] = qr
        qi_v[:, cols] = qi
        q_v[:, cols] = qr.astype(BF)
        q_v[:, more] = qi.astype(BF)

    prepare()
    for j in range(2):
        swaps[j].wait_recv()
        sel[j] = stage[j, tile(c * 64, 64, 64), :] + pbuf[j]
    first = [[], []]
    for k in range(1, 4):
        to, dev = me.xs(k)
        first[0].append(links.go(sel.at[0, :, tile(to * 256, 256, 256)], r0.at[k], dev))
        to, dev = me.ys(k)
        first[1].append(links.go(sel.at[1, tile(to * 16, 16, 16), :], r1.at[k], dev))
    r0[0] = sel[0, :, tile(x * 256, 256, 256)]
    r1[0] = sel[1, tile(y * 16, 16, 16), :]
    split_phases()
    rotate(0)
    for copy in first[0]:
        copy.wait_recv()
    t0[...] = (r0[0] + r0[1]) + (r0[2] + r0[3])
    second = [[], []]
    for k in range(1, 4):
        to, dev = me.ys(k)
        second[0].append(links.go(t0.at[tile(to * 16, 16, 16), :], q0.at[k], dev))
    q0[0] = t0[tile(y * 16, 16, 16), :]
    for copy in first[1]:
        copy.wait_recv()
    t1[...] = (r1[0] + r1[1]) + (r1[2] + r1[3])
    for k in range(1, 4):
        to, dev = me.xs(k)
        second[1].append(links.go(t1.at[:, tile(to * 256, 256, 256)], q1.at[k], dev))
    q1[0] = t1[:, tile(x * 256, 256, 256)]
    rotate(1)
    for copy in second[0]:
        copy.wait_recv()
    zb[0, 0] = (q0[0] + q0[1]) + (q0[2] + q0[3])
    for copy in second[1]:
        copy.wait_recv()
    zb[0, 1] = (q1[0] + q1[1]) + (q1[2] + q1[3])
    third = []
    for k in (4, 3, 5, 2, 6, 1, 7):
        to, dev = me.zs(k)
        third.append(links.go(zb.at[0], zb.at[k], dev))
    rotate(2)
    rotate(3)
    for copy in third:
        copy.wait_recv()
    here = (tile(c * 64 + y * 16, 16, 16), tile(x * 256, 256, 256))
    zeros = jnp.zeros((16, 256), BF)
    for j in range(2):
        half = [zeros, zeros]
        for k in range(8):
            isl = (lax.rem(z - k + 8, 8) < 4).astype(jnp.int32)
            low = isl.astype(F32).astype(BF)
            high = (1 - isl).astype(F32).astype(BF)
            piece = zb[k, j]
            half[0] = half[0] + piece * low
            half[1] = half[1] + piece * high
        for h in range(2):
            cand[h, j, here[0], here[1]] = half[h]
    fourth = [[], []]
    for k in (2, 1, 3):
        spot = cand.at[:, 0, here[0], here[1]]
        fourth[0].append(links.go(spot, spot, me.ys(k)[1]))
        spot = cand.at[:, 1, here[0], here[1]]
        fourth[1].append(links.go(spot, spot, me.xs(k)[1]))
    fifth = [{}, {}]
    forward = []

    def slab0(xx):
        return cand.at[:, 0, tile(c * 64, 64, 64), tile(xx * 256, 256, 256)]

    def slab1(yy):
        return cand.at[:, 1, tile(c * 64 + yy * 16, 16, 16), :]

    oht[...] = (
        lax.broadcasted_iota(jnp.int32, (RELP, 256), 0) == jnp.broadcast_to(rel_r[...], (RELP, 256))
    ).astype(F32).astype(BF)
    for copy in fourth[0]:
        copy.wait_recv()
    for k in (2, 1, 3):
        fifth[0][k] = links.go(slab0(x), slab0(x), me.xs(k)[1])
    for copy in fourth[1]:
        copy.wait_recv()
    for k in (2, 1, 3):
        fifth[1][k] = links.go(slab1(y), slab1(y), me.ys(k)[1])
    forward.append(links.go(slab0(x), slab0(x), me.partner()))
    forward.append(links.go(slab1(y), slab1(y), me.partner()))
    for k in (1, 3, 2):
        fifth[0][k].wait_recv()
        xx = lax.rem(x - k + 4, 4)
        forward.append(links.go(slab0(xx), slab0(xx), me.partner()))
        fifth[1][k].wait_recv()
        yy = lax.rem(y - k + 4, 4)
        forward.append(links.go(slab1(yy), slab1(yy), me.partner()))
    for copy in forward:
        copy.wait_recv()

    for h in range(2):
        for j in range(2):
            block = cand[h, j]
            wide = block.astype(F32)
            norm = jnp.sum(wide * wide, axis=1, keepdims=True)
            inner = lax.dot_general(
                block, q_v[...], (((1,), (1,)), ((), ())), preferred_element_type=F32
            )
            s_v[pl.ds((2 * h + j) * BLK, BLK), :] = inner - norm / SOFTMAX_TEMPER
    scores = s_v[...]
    top = jnp.max(scores, axis=0, keepdims=True)
    log_total = top + jnp.log(jnp.sum(jnp.exp(scores - top), axis=0, keepdims=True))
    mark = (
        lax.broadcasted_iota(jnp.int32, (512, 256), 0) == jnp.broadcast_to(target_r[...], (512, 256))
    )
    loss_o[...] = log_total - jnp.sum(jnp.where(mark, scores, 0.0), axis=0, keepdims=True)
    weights = jnp.exp(scores - log_total) - mark.astype(F32)
    w_v[...] = weights.astype(BF)
    sum_v[...] = jnp.broadcast_to(jnp.sum(weights, axis=1, keepdims=True), (512, 128))

    def back(block):
        rows = tile(block * BLK, BLK, BLK)
        h, j = lax.div(block, 2), lax.rem(block, 2)
        return dot(w_v[rows, :], q_v[...]) - sum_v[rows, 0:1] * cand[h, j].astype(F32)

    for j in range(2):
        asend[pl.ds(j * BLK, BLK), :] = back((1 - c) * 2 + j).astype(BF)
    swap_a = links.go(asend, pa, me.partner())
    for j in range(2):
        afull[pl.ds(j * BLK, BLK), :] = back(c * 2 + j)
    wt_v[...] = jnp.transpose(weights).astype(BF)
    swap_a.wait_recv()
    a1[...] = (afull[...] + pa[...].astype(F32)).astype(BF)
    one_a, one_b = [], []
    for k in (2, 1, 3):
        to, dev = me.xs(k)
        one_a.append(links.go(a1.at[:, tile(to * 256, 256, 256)], ra.at[k - 1], dev))

    for j in range(4):
        cols, more = pl.ds(j * 128, 128), pl.ds(512 + j * 128, 128)
        dqr = dot(wt_v[...], cand[:, :, :, cols].reshape(512, 128))
        dqi = dot(wt_v[...], cand[:, :, :, more].reshape(512, 128))
        cosine, sine = cos_v[:, cols], sin_v[:, cols]
        head_o[:, cols] = (dqr * cosine + dqi * sine).astype(BF)
        head_o[:, more] = (dqi * cosine - dqr * sine).astype(BF)
        angle = dqi * qr_v[:, cols] - dqr * qi_v[:, cols]
        top = angle.astype(BF)
        ang0[:, cols] = top
        ang1[:, cols] = (angle - top.astype(F32)).astype(BF)

    def rel_half(half):
        cols = tile(half * 256, 256, 256)
        return dot(oht[...], ang0[:, cols]) + dot(oht[...], ang1[:, cols])

    bsend[...] = rel_half(1 - c).astype(BF)
    swap_b = links.go(bsend, pb, me.partner())
    bfull[...] = rel_half(c)
    swap_b.wait_recv()
    b1[...] = (bfull[...] + pb[...].astype(F32)).astype(BF)
    for k in (2, 1, 3):
        to, dev = me.ys(k)
        one_b.append(links.go(b1.at[tile(to * RY, RY, 16), :], rb.at[k - 1], dev))
    for copy in one_a:
        copy.wait_recv()
    mine = tile(x * 256, 256, 256)
    total = afull[:, mine] + pa[:, mine].astype(F32)
    for k in range(3):
        total = total + ra[k].astype(F32)
    a2f[...] = total
    a2[...] = total.astype(BF)
    two_a, two_b = [], []
    for k in (2, 1, 3):
        to, dev = me.ys(k)
        two_a.append(links.go(a2.at[tile(to * 64, 64, 64), :], ra2.at[k - 1], dev))
    for copy in one_b:
        copy.wait_recv()
    mine = tile(y * RY, RY, 16)
    total = bfull[mine, :] + pb[mine, :].astype(F32)
    for k in range(3):
        total = total + rb[k].astype(F32)
    b2f[pl.ds(0, RY), :] = total
    b2[pl.ds(0, RY), :] = total.astype(BF)
    b2f[pl.ds(RY, 256 - RY), :] = jnp.zeros((256 - RY, 256), F32)
    b2[pl.ds(RY, 256 - RY), :] = jnp.zeros((256 - RY, 256), BF)
    for k in (2, 1, 3):
        to, dev = me.xs(k)
        two_b.append(links.go(b2.at[tile(to * 64, 64, 64), :], rb2.at[k - 1], dev))

    def zcell(t):
        return tile(lax.div(t, 2) * 16, 16, 16), tile(lax.rem(t, 2) * 128, 128, 128)

    three_a, three_b = [], []
    for copy in two_a:
        copy.wait_recv()
    total = a2f[tile(y * 64, 64, 64), :]
    for k in range(3):
        total = total + ra2[k].astype(F32)
    a3f[...] = total
    a3[...] = total.astype(BF)
    for k in (4, 3, 5, 2, 6, 1, 7):
        to, dev = me.zs(k)
        three_a.append(links.go(a3.at[zcell(to)], raz.at[k - 1], dev))
    for copy in two_b:
        copy.wait_recv()
    total = b2f[tile(x * 64, 64, 64), :]
    for k in range(3):
        total = total + rb2[k].astype(F32)
    b3f[...] = total
    b3[...] = total.astype(BF)
    for k in (4, 3, 5, 2, 6, 1, 7):
        to, dev = me.zs(k)
        three_b.append(links.go(b3.at[zcell(to)], rbz.at[k - 1], dev))

    zr, zc = lax.div(z, 2) * 16, lax.rem(z, 2) * 128

    def a_cell():
        return ga.at[tile(c * 256 + y * 64 + zr, 16, 16), tile(x * 256 + zc, 128, 128)]

    def b_cell():
        return gb.at[y, tile(x * 64 + zr, 16, 16), tile(c * 256 + zc, 128, 128)]

    four_a, four_b = [], []
    for copy in three_a:
        copy.wait_recv()
    total = a3f[zcell(z)]
    for k in range(7):
        total = total + raz[k].astype(F32)
    a_cell()[...] = total.astype(BF)
    for k in (4, 3, 5, 2, 6, 1, 7):
        four_a.append(links.go(a_cell(), a_cell(), me.zs(k)[1]))
    for copy in three_b:
        copy.wait_recv()
    total = b3f[zcell(z)]
    for k in range(7):
        total = total + rbz[k].astype(F32)
    b_cell()[...] = total.astype(BF)
    for k in (4, 3, 5, 2, 6, 1, 7):
        four_b.append(links.go(b_cell(), b_cell(), me.zs(k)[1]))

    five_a, five_b = [], []
    for copy in four_a:
        copy.wait_recv()
    spot = ga.at[tile(c * 256 + y * 64, 64, 64), tile(x * 256, 256, 256)]
    for k in (2, 1, 3):
        five_a.append(links.go(spot, spot, me.ys(k)[1]))
    for copy in four_b:
        copy.wait_recv()
    spot = gb.at[y, tile(x * 64, 64, 64), tile(c * 256, 256, 256)]
    for k in (2, 1, 3):
        five_b.append(links.go(spot, spot, me.xs(k)[1]))

    def slab_a(xx):
        return ga.at[tile(c * 256, 256, 256), tile(xx * 256, 256, 256)]

    def slab_b(yy):
        return gb.at[yy, pl.ds(0, RY), tile(c * 256, 256, 256)]

    six_a, six_b, last = {}, {}, []
    for copy in five_a:
        copy.wait_recv()
    for k in (2, 1, 3):
        six_a[k] = links.go(slab_a(x), slab_a(x), me.xs(k)[1])
    last.append(links.go(slab_a(x), slab_a(x), me.partner()))
    for copy in five_b:
        copy.wait_recv()
    for k in (2, 1, 3):
        six_b[k] = links.go(slab_b(y), slab_b(y), me.ys(k)[1])
    last.append(links.go(slab_b(y), slab_b(y), me.partner()))
    for k in (1, 3, 2):
        six_a[k].wait_recv()
        xx = lax.rem(x - k + 4, 4)
        last.append(links.go(slab_a(xx), slab_a(xx), me.partner()))
        six_b[k].wait_recv()
        yy = lax.rem(y - k + 4, 4)
        last.append(links.go(slab_b(yy), slab_b(yy), me.partner()))
    for copy in last:
        copy.wait_recv()
    links.drain()


def step(owner, local, head, rel, target, table, phases):
    smem = pl.BlockSpec(memory_space=pltpu.SMEM)
    anyw = pl.BlockSpec(memory_space=pl.ANY)
    vmem = pl.BlockSpec(memory_space=pltpu.VMEM)
    shapes = [
        ((512, 1024), BF), ((822, 512), F32), ((128, 512), F32), ((RELK, 512), BF), ((RELK, 512), BF),
        ((RELK, 512), BF), ((256, 512), BF), ((256, RELK), BF), ((256, 1024), BF),
        ((256, 512), F32), ((256, 512), F32), ((256, 512), F32), ((256, 512), F32),
        ((2, 128, 1024), BF), ((2, 64, 1024), BF), ((2, 64, 1024), BF), ((4, 64, 256), BF),
        ((4, 16, 1024), BF), ((64, 256), BF), ((16, 1024), BF), ((4, 16, 256), BF),
        ((4, 16, 256), BF), ((8, 2, 16, 256), BF), ((2, 2, 128, 1024), BF),
        ((512, 256), F32), ((512, 256), BF), ((256, 512), BF), ((512, 128), F32),
        ((256, 512), BF), ((256, 512), BF), ((RELP, 256), BF),
        ((256, 1024), BF), ((256, 1024), F32), ((256, 1024), BF),
        ((RELP, 256), BF), ((RELP, 256), F32), ((RELP, 256), BF),
        ((256, 1024), BF), ((RELP, 256), BF), ((3, 256, 256), BF), ((3, RY, 256), BF),
        ((256, 256), F32), ((256, 256), F32), ((256, 256), BF), ((256, 256), BF),
        ((3, 64, 256), BF), ((3, 64, 256), BF), ((64, 256), F32), ((64, 256), F32),
        ((64, 256), BF), ((64, 256), BF), ((7, 16, 128), BF), ((7, 16, 128), BF),
    ]
    return pl.pallas_call(
        step_kernel,
        out_shape=(
            jax.ShapeDtypeStruct((1, 256), F32),
            jax.ShapeDtypeStruct((256, 1024), BF),
            jax.ShapeDtypeStruct((512, 1024), BF),
            jax.ShapeDtypeStruct((4, 256, 512), BF),
        ),
        in_specs=[smem, smem, vmem, vmem, vmem, anyw, anyw],
        out_specs=(vmem, vmem, vmem, vmem),
        scratch_shapes=[pltpu.VMEM(shape, kind) for shape, kind in shapes]
        + [
            pltpu.SemaphoreType.DMA((N_COPY,)),
            pltpu.SemaphoreType.DMA((N_COPY,)),
            pltpu.SemaphoreType.DMA((2,)),
        ],
        compiler_params=pltpu.CompilerParams(collective_id=0, has_side_effects=True),
    )(owner, local, head, rel, target, table, phases)


def finish_kernel(owner_s, local_s, me_s, loss, head, ga, gb, loss_o, head_o, table_o, rel_o):
    loss_o[...] = loss[...]
    head_o[...] = head[...]
    for n in range(4):
        table_o[pl.ds(n * BLK, BLK), :] = jnp.zeros((BLK, 1024), BF)
        hits = [(owner_s[b] == me_s[0]) & (local_s[b] == n) for b in range(4)]

        @pl.when(hits[0] | hits[1] | hits[2] | hits[3])
        def _():
            total = jnp.zeros((BLK, 1024), F32)
            for b in range(4):
                total = total + ga[pl.ds(b * BLK, BLK), :].astype(F32) * hits[b].astype(F32)
            table_o[pl.ds(n * BLK, BLK), :] = total.astype(BF)

    for k in range(3):
        rel_o[pl.ds(k * RY, RY), :] = gb[k, pl.ds(0, RY), :].astype(F32)
    rel_o[pl.ds(3 * RY, 822 - 3 * RY), :] = gb[3, pl.ds(0, 822 - 3 * RY), :].astype(F32)


def finish(owner, local, entity, loss, head, ga, gb):
    smem = pl.BlockSpec(memory_space=pltpu.SMEM)
    vmem = pl.BlockSpec(memory_space=pltpu.VMEM)
    return pl.pallas_call(
        finish_kernel,
        out_shape=(
            jax.ShapeDtypeStruct((1, 256), F32),
            jax.ShapeDtypeStruct((256, 1024), BF),
            jax.ShapeDtypeStruct((512, 1024), BF),
            jax.ShapeDtypeStruct((822, 512), F32),
        ),
        in_specs=[smem, smem, smem, vmem, vmem, vmem, vmem],
        out_specs=(vmem, vmem, vmem, vmem),
    )(owner, local, entity, loss, head, ga, gb)


def body(entity_table, rel_phases, head_ids, rel_ids, target_pos, block_owner, block_local):
    rows = [ids.reshape(1, 256) for ids in (head_ids, rel_ids, target_pos)]
    loss, head, ga, gb = step(block_owner, block_local, *rows, entity_table, rel_phases)
    entity = lax.axis_index(ENT).astype(jnp.int32).reshape(1)
    loss, head, table, rel = finish(block_owner, block_local, entity, loss, head, ga, gb)
    return loss.reshape(256), head, table, rel


def solution(mesh):
    finer = Mesh(mesh.devices.reshape(4, 4, 4, 2, mesh.shape["grp"]), ENT_GRP)
    placed = (P(ENT, None), P(), P(ENT_GRP), P(ENT_GRP), P(ENT_GRP), P(), P())
    return jax.shard_map(
        body,
        mesh=finer,
        in_specs=placed,
        out_specs=(P(ENT_GRP), P(ENT_GRP, None), P(ENT, None), P()),
        check_vma=False,
    )
```
